32 devices in a mesh: seq: 4 (over z), tensor: 2 (over x), dp: 4 (over y, core).
Axes of the slice: x: 2, y: 2, z: 4, core: 2. Of those that a mesh axis runs over, the one named last changes fastest.
Arguments:
- tokens: bfloat16 [4, 1024, 3072], P('dp', 'seq'), may hold values from -6 to 6
- cotangent: bfloat16 [4, 1024, 3072], P('dp', 'seq'), may hold values from -6 to 6
- qkv_weight: bfloat16 [3072, 3, 768], P(('seq', 'dp'), None, 'tensor'), may hold values from -0.109375 to 0.109375
- out_weight: bfloat16 [3072, 768], P(('seq', 'dp'), 'tensor'), may hold values from -0.21875 to 0.21875
Outputs:
- qkv_grad: float32 [3072, 3, 768], P(('seq', 'dp'), None, 'tensor')
- out_grad: float32 [3072, 768], P(('seq', 'dp'), 'tensor')
- branch_grad: bfloat16 [4, 1024, 3072], P('dp', 'seq', 'tensor')
The draws below stay inside these ranges and needn't reach their ends.
All inputs are finite; a program needn't handle non-finite values.
Results may differ from the reference program's by a relative error of at most 0.025.
Values may be sent and summed in bfloat16 or wider, within the bound.
A program may use at most 128 MiB of HBM per device.

```python
import jax
import jax.numpy as jnp
from jax import lax

D = 3072
HD = 128
TOK_DEV = 256
HEADS = 6
SEQ_LEN = 1024
BATCH = 4
N_SEQ = 4


def strengthened(drawn, key, source, target, blocks, factor):
    def block_of(axis_at):
        return (jnp.arange(drawn.shape[axis_at]) // (drawn.shape[axis_at] // blocks)).reshape((-1,) + (1,) * (drawn.ndim - 1 - axis_at))

    near = jax.random.permutation(key, blocks)[block_of(target)]
    second = (block_of(target) + blocks // 2) % blocks
    return jnp.where((block_of(source) == near) | (block_of(source) == second), factor * drawn, drawn)


def block_scale(stream_key, dims, shards, low, largest):
    loudness = 1.0
    for axis_at, blocks in shards:
        draws = jax.random.uniform(jax.random.fold_in(jax.random.fold_in(stream_key, 6), axis_at), (blocks,), jnp.float32, low / len(shards), largest / len(shards))
        loudness = loudness * jnp.repeat(jnp.exp(draws), dims[axis_at] // blocks).reshape((-1,) + (1,) * (len(dims) - 1 - axis_at))
    return loudness


def bell_draw(stream_key, extent, scale, most, split=(), held_as=jnp.bfloat16):
    values = jax.random.normal(stream_key, extent, jnp.float32) * scale
    if len(split) > 0:
        values = block_scale(stream_key, extent, split, -0.22, 0.18) * values
    return jnp.clip(values, min=-most, max=most).astype(held_as)


def bell_draw_with(rng, extent, scale, reach, shards, heavy, kind=jnp.bfloat16):
    result = scale * jax.random.normal(rng, extent, jnp.float32)
    if shards:
        result = result * block_scale(rng, extent, shards, -0.22, 0.18)
    return jnp.clip(strengthened(result, jax.random.fold_in(rng, 3), *heavy), -reach, reach).astype(kind)


def setup_inputs(seed: int = 0) -> dict:
    seeds = jax.random.split(jax.random.key(seed), 5)
    return {
        "tokens": bell_draw_with(seeds[0], (BATCH, SEQ_LEN, D), 1.0, 6.0, ((0, 4), (1, 4)), (1, 2, 4, 2.0)),
        "cotangent": bell_draw_with(seeds[1], (BATCH, SEQ_LEN, D), 1.0, 6.0, ((0, 4), (1, 4)), (1, 2, 4, 2.0)),
        "qkv_weight": bell_draw(seeds[2], (D, 3, HEADS * HD), D ** -0.5, 0.109375, ((0, 16), (2, 2))),
        "out_weight": bell_draw(seeds[3], (D, HEADS * HD), (HEADS * HD) ** -0.5, 0.21875, ((0, 16), (1, 2))),
    }


epsilon = 1e-06

def normalize(values):
    average = lax.optimization_barrier(jnp.mean(values, axis=-1, keepdims=True))
    centered = values - average
    inverse = lax.rsqrt(lax.optimization_barrier(jnp.mean(centered * centered, axis=-1, keepdims=True)) + epsilon)
    return (centered * inverse, inverse)

def normalize_back(gradient, normed, inverse):
    mean_grad = lax.optimization_barrier(jnp.mean(gradient, axis=-1, keepdims=True))
    mean_both = lax.optimization_barrier(jnp.mean(gradient * normed, axis=-1, keepdims=True))
    return (gradient - mean_grad - normed * mean_both) * inverse

def narrow(values):
    return lax.optimization_barrier(values.astype(jnp.bfloat16)).astype(jnp.float32)

def reference(tokens, cotangent, qkv_weight, out_weight):
    all_columns = HEADS * HD
    score_scale = HD ** (-0.5)
    flat_weight = qkv_weight.reshape(D, 3 * all_columns)
    qkv_total = jnp.zeros((D, 3 * all_columns), jnp.float32)
    out_total = jnp.zeros((D, all_columns), jnp.float32)
    branches = []
    for batch_row in range(BATCH):
        row_grads = cotangent[batch_row]
        normed, inverse = normalize(tokens[batch_row].astype(jnp.float32))
        unit_low = normed.astype(jnp.bfloat16)
        projected = jnp.dot(unit_low, flat_weight, preferred_element_type=jnp.float32)
        query_unit, query_inv = normalize(projected[:, :all_columns].reshape(SEQ_LEN, HEADS, HD))
        key_unit, key_inv = normalize(projected[:, all_columns:2 * all_columns].reshape(SEQ_LEN, HEADS, HD))
        query_low = narrow(query_unit)
        key_low = narrow(key_unit)
        value_low = narrow(projected[:, 2 * all_columns:].reshape(SEQ_LEN, HEADS, HD))
        scores = jnp.einsum('qhd,khd->hqk', query_low, key_low) * score_scale
        exponent = jnp.exp(scores)
        exp_total = lax.optimization_barrier(jnp.sum(exponent, axis=-1))
        attended = jnp.einsum('hqk,khd->qhd', narrow(exponent), value_low) / exp_total.T[:, :, None]
        attended_low = attended.astype(jnp.bfloat16)
        attended_wide = lax.optimization_barrier(attended_low).astype(jnp.float32)
        grad_low = jnp.dot(row_grads, out_weight, preferred_element_type=jnp.float32).astype(jnp.bfloat16)
        grad_wide = lax.optimization_barrier(grad_low).astype(jnp.float32).reshape(SEQ_LEN, HEADS, HD)
        row_delta = lax.optimization_barrier(jnp.sum(grad_wide * attended_wide, axis=-1))
        probability = exponent / exp_total[:, :, None]
        prob_grad = jnp.einsum('qhd,khd->hqk', grad_wide, value_low)
        grad_score = narrow(probability * (prob_grad - row_delta.T[:, :, None]) * score_scale)
        query_raw = jnp.einsum('hqk,khd->qhd', grad_score, key_low)
        key_raw = jnp.einsum('hqk,qhd->khd', grad_score, query_low)
        value_raw = jnp.einsum('hqk,qhd->khd', narrow(probability), grad_wide)
        query_back = normalize_back(query_raw, query_unit, query_inv)
        key_back = normalize_back(key_raw, key_unit, key_inv)
        qkv_low = jnp.concatenate([query_back.reshape(SEQ_LEN, all_columns), key_back.reshape(SEQ_LEN, all_columns), value_raw.reshape(SEQ_LEN, all_columns)], axis=1).astype(jnp.bfloat16)
        inner_grad = jnp.dot(qkv_low, flat_weight.T, preferred_element_type=jnp.float32)
        branches.append(normalize_back(inner_grad, normed, inverse).astype(jnp.bfloat16))
        attended_flat = attended_low.reshape(SEQ_LEN, all_columns)
        for block_index in range(N_SEQ):
            low_row = block_index * TOK_DEV
            high_row = low_row + TOK_DEV
            qkv_total = qkv_total + narrow(jnp.dot(unit_low[low_row:high_row].T, qkv_low[low_row:high_row], preferred_element_type=jnp.float32))
            out_total = out_total + narrow(jnp.dot(row_grads[low_row:high_row].T, attended_flat[low_row:high_row], preferred_element_type=jnp.float32))
    return (qkv_total.reshape(D, 3, all_columns), out_total, jnp.stack(branches))
```

```python
import functools

import jax
import jax.numpy as jnp
from jax import lax
from jax.experimental import pallas as pl
from jax.experimental.pallas import tpu as pltpu
from jax.sharding import PartitionSpec as P

HD = 128

CORES = 2
CHUNKS = 2
MESH_ID = pl.DeviceIdType.MESH


def greet(seq_count, chip_count, place, chip, core):
    barrier = pltpu.get_barrier_semaphore()

    def signal(device):
        pl.semaphore_signal(barrier, inc=1, device_id=device, device_id_type=MESH_ID)

    @pl.when(place > 0)
    def _():
        signal({"seq": place - 1})

    @pl.when(place < seq_count - 1)
    def _():
        signal({"seq": place + 1})

    for step in range(1, chip_count):
        signal({"dp": (chip + step) % chip_count * CORES + core})
    signal({"dp": chip * CORES + 1 - core})
    ends = jnp.minimum(place, 1) + jnp.minimum(seq_count - 1 - place, 1)
    pl.semaphore_wait(barrier, chip_count + ends)


def gather_kernel(
    seq_count, dp_count, own_ref, out_ref, recv, right_sem, left_sem, chip_sem, core_sem, own_sem
):
    chip_count = dp_count // CORES
    place = lax.axis_index("seq")
    index = lax.axis_index("dp")
    chip, core = index // CORES, index % CORES
    greet(seq_count, chip_count, place, chip, core)
    own_copy = pltpu.make_async_copy(own_ref, out_ref.at[place * dp_count + index], own_sem)
    own_copy.start()

    def copy(source, slot, send_sem, device):
        return pltpu.make_async_remote_copy(
            src_ref=source,
            dst_ref=out_ref.at[slot],
            send_sem=send_sem,
            recv_sem=recv.at[slot],
            device_id=device,
            device_id_type=MESH_ID,
        )

    def right(source, origin):
        return copy(
            source, origin * dp_count + index, right_sem.at[origin], {"seq": place + 1}
        )

    def left(source, origin):
        return copy(source, origin * dp_count + index, left_sem.at[origin], {"seq": place - 1})

    def across(source, origin, step):
        return copy(
            source,
            origin * dp_count + index,
            chip_sem.at[origin * chip_count + step],
            {"dp": (chip + step) % chip_count * CORES + core},
        )

    def beside(source, origin, source_chip):
        return copy(
            source,
            origin * dp_count + source_chip * CORES + core,
            core_sem.at[origin * chip_count + source_chip],
            {"dp": chip * CORES + 1 - core},
        )

    def landed(slot):
        copy(own_ref, slot, core_sem.at[0], {"dp": chip * CORES + 1 - core}).wait_recv()

    def spread(source, origin):
        for step in range(1, chip_count):
            across(source, origin, step).start()
        beside(source, origin, chip).start()

    @pl.when(place < seq_count - 1)
    def _():
        right(own_ref, place).start()

    @pl.when(place > 0)
    def _():
        left(own_ref, place).start()

    spread(own_ref, place)
    for step in range(1, seq_count):
        low, high = place - step, place + step

        @pl.when(low >= 0)
        def _():
            slot = low * dp_count + index
            landed(slot)

            @pl.when(place < seq_count - 1)
            def _():
                right(out_ref.at[slot], low).start()

            spread(out_ref.at[slot], low)

        @pl.when(high < seq_count)
        def _():
            slot = high * dp_count + index
            landed(slot)

            @pl.when(place > 0)
            def _():
                left(out_ref.at[slot], high).start()

            spread(out_ref.at[slot], high)

    for turn in range(seq_count):
        origin = (place + turn) % seq_count
        for step in range(1, chip_count):
            source_chip = (chip + step) % chip_count
            slot = origin * dp_count + source_chip * CORES + core
            landed(slot)
            beside(out_ref.at[slot], origin, source_chip).start()
    for origin in range(seq_count):
        for source_chip in range(chip_count):
            landed(origin * dp_count + source_chip * CORES + 1 - core)
    own_copy.wait()
    for origin in range(seq_count):
        for step in range(1, chip_count):
            across(own_ref, origin, step).wait_send()
        for source_chip in range(chip_count):
            beside(own_ref, origin, source_chip).wait_send()

        @pl.when((origin <= place) & (place < seq_count - 1))
        def _():
            right(own_ref, origin).wait_send()

        @pl.when((origin >= place) & (place > 0))
        def _():
            left(own_ref, origin).wait_send()


def gather_rows(own):
    seq_count, dp_count = lax.axis_size("seq"), lax.axis_size("dp")
    chip_count = dp_count // CORES
    return pl.pallas_call(
        functools.partial(gather_kernel, seq_count, dp_count),
        out_shape=jax.ShapeDtypeStruct((seq_count * dp_count,) + own.shape, own.dtype),
        in_specs=[pl.BlockSpec(memory_space=pltpu.VMEM)],
        out_specs=pl.BlockSpec(memory_space=pl.ANY),
        scratch_shapes=[
            pltpu.SemaphoreType.DMA((seq_count * dp_count,)),
            pltpu.SemaphoreType.DMA((seq_count,)),
            pltpu.SemaphoreType.DMA((seq_count,)),
            pltpu.SemaphoreType.DMA((seq_count * chip_count,)),
            pltpu.SemaphoreType.DMA((seq_count * chip_count,)),
            pltpu.SemaphoreType.DMA,
        ],
        compiler_params=pltpu.CompilerParams(collective_id=0, has_side_effects=True),
        cost_estimate=pl.CostEstimate(flops=0, bytes_accessed=150000000, transcendentals=0),
        name="gather_rows",
    )(own)


epsilon = 1e-06


def normalize(values):
    average = jnp.mean(values, axis=-1, keepdims=True)
    centered = values - average
    inverse = lax.rsqrt(jnp.mean(centered * centered, axis=-1, keepdims=True) + epsilon)
    return (centered * inverse, inverse)


def normalize_back(gradient, normed, inverse):
    mean_grad = jnp.mean(gradient, axis=-1, keepdims=True)
    mean_both = jnp.mean(gradient * normed, axis=-1, keepdims=True)
    return (gradient - mean_grad - normed * mean_both) * inverse


def local(tokens, cotangent, qkv_weight, out_weight):
    row_count = tokens.shape[1]
    feature_count = tokens.shape[2]
    column_count = out_weight.shape[1]
    head_count = column_count // HD
    score_scale = HD ** (-0.5)
    own_rows = qkv_weight.shape[0]
    grad_rows = cotangent[0]
    normed, inverse = normalize(tokens[0].astype(jnp.float32))
    unit_low = normed.astype(jnp.bfloat16)
    flat_weight = qkv_weight.reshape(own_rows, 3 * column_count)
    piece_all = gather_rows(jnp.concatenate([flat_weight, out_weight], axis=1)).reshape(
        feature_count, 4 * column_count
    )
    piece_qkv = piece_all[:, : 3 * column_count]
    piece_out = piece_all[:, 3 * column_count :]
    piece_rows = piece_qkv.shape[0]
    left_rows = unit_low
    right_rows = grad_rows
    projected = jnp.dot(left_rows, piece_qkv, preferred_element_type=jnp.float32)
    attended_grad = jnp.dot(right_rows, piece_out, preferred_element_type=jnp.float32)
    full_qkv = piece_qkv
    projected, attended_grad, full_qkv = (projected, attended_grad, full_qkv)
    query_unit, query_inv = normalize(
        projected[:, :column_count].reshape(row_count, head_count, HD)
    )
    key_unit, key_inv = normalize(
        projected[:, column_count : 2 * column_count].reshape(row_count, head_count, HD)
    )
    query_low = query_unit.astype(jnp.bfloat16)
    key_value = jnp.stack(
        [
            key_unit.astype(jnp.bfloat16).reshape(row_count, column_count),
            projected[:, 2 * column_count :].astype(jnp.bfloat16),
        ]
    )
    grad_low = attended_grad.astype(jnp.bfloat16).reshape(row_count, head_count, HD)

    def scores_of(key_rows):
        piece_rows = key_rows.shape[0]
        return (
            jnp.einsum(
                "qhd,khd->hqk",
                query_low,
                key_rows.reshape(piece_rows, head_count, HD),
                preferred_element_type=jnp.float32,
            )
            * score_scale
        )

    every_pair = lax.all_gather(key_value, "seq", axis=1, tiled=True)
    piece_rows = every_pair.shape[1]
    exponent = jnp.exp(scores_of(every_pair[0]))
    add_exp_total = jnp.sum(exponent, axis=-1)
    weighted = jnp.einsum(
        "hqk,khd->qhd",
        exponent.astype(jnp.bfloat16),
        every_pair[1].reshape(piece_rows, head_count, HD),
        preferred_element_type=jnp.float32,
    )
    exp_total, weighted = (add_exp_total, weighted)
    attended_low = (weighted / exp_total.T[:, :, None]).astype(jnp.bfloat16)
    row_delta = jnp.sum(grad_low.astype(jnp.float32) * attended_low.astype(jnp.float32), axis=-1)
    piece_rows = every_pair.shape[1]
    key_rows = every_pair[0].reshape(piece_rows, head_count, HD)
    value_rows = every_pair[1].reshape(piece_rows, head_count, HD)
    probability = jnp.exp(scores_of(every_pair[0])) / exp_total[:, :, None]
    prob_grad = jnp.einsum("qhd,khd->hqk", grad_low, value_rows, preferred_element_type=jnp.float32)
    grad_score = (probability * (prob_grad - row_delta.T[:, :, None]) * score_scale).astype(
        jnp.bfloat16
    )
    query_part = jnp.einsum(
        "hqk,khd->qhd", grad_score, key_rows, preferred_element_type=jnp.float32
    )
    key_part = jnp.einsum("hqk,qhd->khd", grad_score, query_low, preferred_element_type=jnp.float32)
    value_part = jnp.einsum(
        "hqk,qhd->khd",
        probability.astype(jnp.bfloat16),
        grad_low,
        preferred_element_type=jnp.float32,
    )
    every_grad = jnp.stack(
        [key_part.reshape(piece_rows, column_count), value_part.reshape(piece_rows, column_count)]
    )
    pair_grad = lax.psum_scatter(
        every_grad.astype(jnp.bfloat16), "seq", scatter_dimension=1, tiled=True
    ).astype(jnp.float32)
    query_back = normalize_back(query_part, query_unit, query_inv)
    key_back = normalize_back(pair_grad[0].reshape(row_count, head_count, HD), key_unit, key_inv)
    qkv_low = jnp.concatenate(
        [
            query_back.reshape(row_count, column_count),
            key_back.reshape(row_count, column_count),
            pair_grad[1],
        ],
        axis=1,
    ).astype(jnp.bfloat16)
    inner_grad = jnp.einsum("rc,dc->rd", qkv_low, full_qkv, preferred_element_type=jnp.float32)
    attended_flat = attended_low.reshape(row_count, column_count)
    share_width = feature_count // lax.axis_size("tensor")
    whole_sum = lax.psum(inner_grad.astype(jnp.bfloat16), "tensor").astype(jnp.float32)
    branch = lax.dynamic_slice_in_dim(
        normalize_back(whole_sum, normed, inverse),
        lax.axis_index("tensor") * share_width,
        share_width,
        1,
    )
    left_rows = unit_low
    right_rows = grad_rows
    qkv_term = jnp.einsum(
        "rd,rc->dc", left_rows, qkv_low, preferred_element_type=jnp.float32
    ).reshape(lax.axis_size(("seq", "dp")) * own_rows, 3, column_count)
    out_term = jnp.einsum(
        "rd,rc->dc", right_rows, attended_flat, preferred_element_type=jnp.float32
    )
    summed = lax.psum_scatter(
        jnp.concatenate([qkv_term, out_term[:, None, :]], axis=1).astype(jnp.bfloat16),
        ("seq", "dp"),
        scatter_dimension=0,
        tiled=True,
    ).astype(jnp.float32)
    return (summed[:, :3], summed[:, 3], branch.astype(jnp.bfloat16)[None])


def solution(mesh):
    return jax.shard_map(
        local,
        mesh=mesh,
        in_specs=(
            P("dp", "seq", None),
            P("dp", "seq", None),
            P(("seq", "dp"), None, "tensor"),
            P(("seq", "dp"), "tensor"),
        ),
        out_specs=(
            P(("seq", "dp"), None, "tensor"),
            P(("seq", "dp"), "tensor"),
            P("dp", "seq", "tensor"),
        ),
        check_vma=False,
    )
```

```python
import functools

import jax
import jax.numpy as jnp
from jax import lax
from jax.experimental import pallas as pl
from jax.experimental.pallas import tpu as pltpu
from jax.sharding import PartitionSpec as P

HD = 128

CORES = 2
CHUNKS = 2
MESH_ID = pl.DeviceIdType.MESH


def greet(seq_count, chip_count, place, chip, core):
    barrier = pltpu.get_barrier_semaphore()

    def signal(device):
        pl.semaphore_signal(barrier, inc=1, device_id=device, device_id_type=MESH_ID)

    @pl.when(place > 0)
    def _():
        signal({"seq": place - 1})

    @pl.when(place < seq_count - 1)
    def _():
        signal({"seq": place + 1})

    for step in range(1, chip_count):
        signal({"dp": (chip + step) % chip_count * CORES + core})
    signal({"dp": chip * CORES + 1 - core})
    ends = jnp.minimum(place, 1) + jnp.minimum(seq_count - 1 - place, 1)
    pl.semaphore_wait(barrier, chip_count + ends)


def gather_kernel(
    seq_count, dp_count, own_ref, out_ref, recv, right_sem, left_sem, chip_sem, core_sem, own_sem
):
    chip_count = dp_count // CORES
    place = lax.axis_index("seq")
    index = lax.axis_index("dp")
    chip, core = index // CORES, index % CORES
    greet(seq_count, chip_count, place, chip, core)
    own_copy = pltpu.make_async_copy(own_ref, out_ref.at[place * dp_count + index], own_sem)
    own_copy.start()

    def copy(source, slot, send_sem, device):
        return pltpu.make_async_remote_copy(
            src_ref=source,
            dst_ref=out_ref.at[slot],
            send_sem=send_sem,
            recv_sem=recv.at[slot],
            device_id=device,
            device_id_type=MESH_ID,
        )

    def right(source, origin):
        return copy(
            source, origin * dp_count + index, right_sem.at[origin], {"seq": place + 1}
        )

    def left(source, origin):
        return copy(source, origin * dp_count + index, left_sem.at[origin], {"seq": place - 1})

    def across(source, origin, step):
        return copy(
            source,
            origin * dp_count + index,
            chip_sem.at[origin * chip_count + step],
            {"dp": (chip + step) % chip_count * CORES + core},
        )

    def beside(source, origin, source_chip):
        return copy(
            source,
            origin * dp_count + source_chip * CORES + core,
            core_sem.at[origin * chip_count + source_chip],
            {"dp": chip * CORES + 1 - core},
        )

    def landed(slot):
        copy(own_ref, slot, core_sem.at[0], {"dp": chip * CORES + 1 - core}).wait_recv()

    def spread(source, origin):
        for step in range(1, chip_count):
            across(source, origin, step).start()
        beside(source, origin, chip).start()

    @pl.when(place < seq_count - 1)
    def _():
        right(own_ref, place).start()

    @pl.when(place > 0)
    def _():
        left(own_ref, place).start()

    spread(own_ref, place)
    for step in range(1, seq_count):
        low, high = place - step, place + step

        @pl.when(low >= 0)
        def _():
            slot = low * dp_count + index
            landed(slot)

            @pl.when(place < seq_count - 1)
            def _():
                right(out_ref.at[slot], low).start()

            spread(out_ref.at[slot], low)

        @pl.when(high < seq_count)
        def _():
            slot = high * dp_count + index
            landed(slot)

            @pl.when(place > 0)
            def _():
                left(out_ref.at[slot], high).start()

            spread(out_ref.at[slot], high)

    for turn in range(seq_count):
        origin = (place + turn) % seq_count
        for step in range(1, chip_count):
            source_chip = (chip + step) % chip_count
            slot = origin * dp_count + source_chip * CORES + core
            landed(slot)
            beside(out_ref.at[slot], origin, source_chip).start()
    for origin in range(seq_count):
        for source_chip in range(chip_count):
            landed(origin * dp_count + source_chip * CORES + 1 - core)
    own_copy.wait()
    for origin in range(seq_count):
        for step in range(1, chip_count):
            across(own_ref, origin, step).wait_send()
        for source_chip in range(chip_count):
            beside(own_ref, origin, source_chip).wait_send()

        @pl.when((origin <= place) & (place < seq_count - 1))
        def _():
            right(own_ref, origin).wait_send()

        @pl.when((origin >= place) & (place > 0))
        def _():
            left(own_ref, origin).wait_send()


def gather_rows(own):
    seq_count, dp_count = lax.axis_size("seq"), lax.axis_size("dp")
    chip_count = dp_count // CORES
    return pl.pallas_call(
        functools.partial(gather_kernel, seq_count, dp_count),
        out_shape=jax.ShapeDtypeStruct((seq_count * dp_count,) + own.shape, own.dtype),
        in_specs=[pl.BlockSpec(memory_space=pltpu.VMEM)],
        out_specs=pl.BlockSpec(memory_space=pl.ANY),
        scratch_shapes=[
            pltpu.SemaphoreType.DMA((seq_count * dp_count,)),
            pltpu.SemaphoreType.DMA((seq_count,)),
            pltpu.SemaphoreType.DMA((seq_count,)),
            pltpu.SemaphoreType.DMA((seq_count * chip_count,)),
            pltpu.SemaphoreType.DMA((seq_count * chip_count,)),
            pltpu.SemaphoreType.DMA,
        ],
        compiler_params=pltpu.CompilerParams(collective_id=0, has_side_effects=True),
        cost_estimate=pl.CostEstimate(flops=0, bytes_accessed=150000000, transcendentals=0),
        name="gather_rows",
    )(own)

def scatter_kernel(
    seq_count,
    dp_count,
    term_ref,
    out_ref,
    held,
    chip_in,
    low_in,
    high_in,
    core_recv,
    core_send,
    chip_recv,
    chip_send,
    low_recv,
    high_recv,
    chain_send,
):
    chip_count = dp_count // CORES
    part_rows = term_ref.shape[1] // CHUNKS
    place = lax.axis_index("seq")
    index = lax.axis_index("dp")
    chip, core = index // CORES, index % CORES
    greet(seq_count, chip_count, place, chip, core)

    def piece(ref, slot, part):
        return ref.at[slot, pl.ds(part * part_rows, part_rows)]

    def copy(source, target_ref, part, slot, send_sem, recv_sem, device):
        return pltpu.make_async_remote_copy(
            src_ref=source,
            dst_ref=piece(target_ref, slot, part),
            send_sem=send_sem.at[slot * CHUNKS + part],
            recv_sem=recv_sem.at[slot * CHUNKS + part],
            device_id=device,
            device_id_type=MESH_ID,
        )

    def beside(part, target, target_chip):
        source = piece(term_ref, target * dp_count + target_chip * CORES + 1 - core, part)
        slot = target * chip_count + target_chip
        device = {"dp": chip * CORES + 1 - core}
        return copy(source, held, part, slot, core_send, core_recv, device)

    def across(part, target, step):
        other = (chip + step) % chip_count
        source = piece(held, target * chip_count + other, part)
        slot = (step - 1) * seq_count + target
        device = {"dp": other * CORES + core}
        return copy(source, chip_in, part, slot, chip_send, chip_recv, device)

    def upward(part, target):
        source = piece(held, target * chip_count + chip, part)
        return copy(source, low_in, part, target, chain_send, low_recv, {"seq": place + 1})

    def downward(part, target):
        source = piece(held, target * chip_count + chip, part)
        return copy(source, high_in, part, target, chain_send, high_recv, {"seq": place - 1})

    def add(slot, part, others):
        @pl.loop(0, part_rows // 16)
        def _(step):
            rows = pl.ds(pl.multiple_of(part * part_rows + step * 16, 16), 16)
            total = held[slot, rows, :].astype(jnp.float32)
            for ref, other in others:
                total = total + ref[other, rows, :].astype(jnp.float32)
            held[slot, rows, :] = total.astype(held.dtype)

    order = []
    for turn in range((seq_count + 1) // 2):
        order.extend(sorted({seq_count - 1 - turn, turn}, reverse=True))
    items = [(part, target) for part in range(CHUNKS) for target in order]
    for part, target in items:
        for step in range(1, chip_count):
            beside(part, target, (chip + step) % chip_count).start()
    for part, target in items:
        beside(part, target, chip).start()
    for part, target in items:
        for step in range(1, chip_count):
            other = (chip + step) % chip_count
            beside(part, target, other).wait_recv()
            own_slot = target * dp_count + other * CORES + core
            add(target * chip_count + other, part, [(term_ref, own_slot)])
            across(part, target, step).start()
    for part, target in items:
        slot = target * chip_count + chip
        others = [(term_ref, target * dp_count + index)]
        beside(part, target, chip).wait_recv()
        for step in range(1, chip_count):
            across(part, target, step).wait_recv()
            others.append((chip_in, (step - 1) * seq_count + target))
        add(slot, part, others)
        if target > 0:

            @pl.when(place < target)
            def _():
                @pl.when(place > 0)
                def _():
                    upward(part, target).wait_recv()
                    add(slot, part, [(low_in, target)])

                upward(part, target).start()

        if target < seq_count - 1:

            @pl.when(place > target)
            def _():
                @pl.when(place < seq_count - 1)
                def _():
                    downward(part, target).wait_recv()
                    add(slot, part, [(high_in, target)])

                downward(part, target).start()

    out_ref[...] = held[place * chip_count + chip].astype(jnp.float32)

    @pl.when(place > 0)
    def _():
        for part in range(CHUNKS):
            upward(part, place).wait_recv()
        out_ref[...] += low_in[place].astype(jnp.float32)

    @pl.when(place < seq_count - 1)
    def _():
        for part in range(CHUNKS):
            downward(part, place).wait_recv()
        out_ref[...] += high_in[place].astype(jnp.float32)

    for part, target in items:
        for step in range(1, chip_count):
            across(part, target, step).wait_send()
        for target_chip in range(chip_count):
            beside(part, target, target_chip).wait_send()

        @pl.when(place != target)
        def _():
            upward(part, target).wait_send()


def scatter_rows(terms):
    seq_count, dp_count = lax.axis_size("seq"), lax.axis_size("dp")
    chip_count = dp_count // CORES
    shape = terms.shape[1:]

    def slots(count):
        return pltpu.VMEM((count,) + shape, terms.dtype)

    def semaphores(count):
        return pltpu.SemaphoreType.DMA((count * CHUNKS,))

    both, peers = seq_count * chip_count, seq_count * (chip_count - 1)
    return pl.pallas_call(
        functools.partial(scatter_kernel, seq_count, dp_count),
        out_shape=jax.ShapeDtypeStruct(shape, jnp.float32),
        in_specs=[pl.BlockSpec(memory_space=pltpu.VMEM)],
        out_specs=pl.BlockSpec(memory_space=pltpu.VMEM),
        scratch_shapes=[
            slots(both),
            slots(peers),
            slots(seq_count),
            slots(seq_count),
            semaphores(both),
            semaphores(both),
            semaphores(peers),
            semaphores(peers),
            semaphores(seq_count),
            semaphores(seq_count),
            semaphores(seq_count),
        ],
        compiler_params=pltpu.CompilerParams(
            collective_id=1, has_side_effects=True, vmem_limit_bytes=40 * 1024 * 1024
        ),
        cost_estimate=pl.CostEstimate(flops=0, bytes_accessed=180000000, transcendentals=0),
        name="scatter_rows",
    )(terms)


epsilon = 1e-06


def normalize(values):
    average = jnp.mean(values, axis=-1, keepdims=True)
    centered = values - average
    inverse = lax.rsqrt(jnp.mean(centered * centered, axis=-1, keepdims=True) + epsilon)
    return (centered * inverse, inverse)


def normalize_back(gradient, normed, inverse):
    mean_grad = jnp.mean(gradient, axis=-1, keepdims=True)
    mean_both = jnp.mean(gradient * normed, axis=-1, keepdims=True)
    return (gradient - mean_grad - normed * mean_both) * inverse


def local(tokens, cotangent, qkv_weight, out_weight):
    row_count = tokens.shape[1]
    feature_count = tokens.shape[2]
    column_count = out_weight.shape[1]
    head_count = column_count // HD
    score_scale = HD ** (-0.5)
    own_rows = qkv_weight.shape[0]
    grad_rows = cotangent[0]
    normed, inverse = normalize(tokens[0].astype(jnp.float32))
    unit_low = normed.astype(jnp.bfloat16)
    flat_weight = qkv_weight.reshape(own_rows, 3 * column_count)
    piece_all = gather_rows(jnp.concatenate([flat_weight, out_weight], axis=1)).reshape(
        feature_count, 4 * column_count
    )
    piece_qkv = piece_all[:, : 3 * column_count]
    piece_out = piece_all[:, 3 * column_count :]
    piece_rows = piece_qkv.shape[0]
    left_rows = unit_low
    right_rows = grad_rows
    projected = jnp.dot(left_rows, piece_qkv, preferred_element_type=jnp.float32)
    attended_grad = jnp.dot(right_rows, piece_out, preferred_element_type=jnp.float32)
    full_qkv = piece_qkv
    projected, attended_grad, full_qkv = (projected, attended_grad, full_qkv)
    query_unit, query_inv = normalize(
        projected[:, :column_count].reshape(row_count, head_count, HD)
    )
    key_unit, key_inv = normalize(
        projected[:, column_count : 2 * column_count].reshape(row_count, head_count, HD)
    )
    query_low = query_unit.astype(jnp.bfloat16)
    key_value = jnp.stack(
        [
            key_unit.astype(jnp.bfloat16).reshape(row_count, column_count),
            projected[:, 2 * column_count :].astype(jnp.bfloat16),
        ]
    )
    grad_low = attended_grad.astype(jnp.bfloat16).reshape(row_count, head_count, HD)

    def scores_of(key_rows):
        piece_rows = key_rows.shape[0]
        return (
            jnp.einsum(
                "qhd,khd->hqk",
                query_low,
                key_rows.reshape(piece_rows, head_count, HD),
                preferred_element_type=jnp.float32,
            )
            * score_scale
        )

    every_pair = lax.all_gather(key_value, "seq", axis=1, tiled=True)
    piece_rows = every_pair.shape[1]
    exponent = jnp.exp(scores_of(every_pair[0]))
    add_exp_total = jnp.sum(exponent, axis=-1)
    weighted = jnp.einsum(
        "hqk,khd->qhd",
        exponent.astype(jnp.bfloat16),
        every_pair[1].reshape(piece_rows, head_count, HD),
        preferred_element_type=jnp.float32,
    )
    exp_total, weighted = (add_exp_total, weighted)
    attended_low = (weighted / exp_total.T[:, :, None]).astype(jnp.bfloat16)
    row_delta = jnp.sum(grad_low.astype(jnp.float32) * attended_low.astype(jnp.float32), axis=-1)
    piece_rows = every_pair.shape[1]
    key_rows = every_pair[0].reshape(piece_rows, head_count, HD)
    value_rows = every_pair[1].reshape(piece_rows, head_count, HD)
    probability = jnp.exp(scores_of(every_pair[0])) / exp_total[:, :, None]
    prob_grad = jnp.einsum("qhd,khd->hqk", grad_low, value_rows, preferred_element_type=jnp.float32)
    grad_score = (probability * (prob_grad - row_delta.T[:, :, None]) * score_scale).astype(
        jnp.bfloat16
    )
    query_part = jnp.einsum(
        "hqk,khd->qhd", grad_score, key_rows, preferred_element_type=jnp.float32
    )
    key_part = jnp.einsum("hqk,qhd->khd", grad_score, query_low, preferred_element_type=jnp.float32)
    value_part = jnp.einsum(
        "hqk,qhd->khd",
        probability.astype(jnp.bfloat16),
        grad_low,
        preferred_element_type=jnp.float32,
    )
    every_grad = jnp.stack(
        [key_part.reshape(piece_rows, column_count), value_part.reshape(piece_rows, column_count)]
    )
    pair_grad = lax.psum_scatter(
        every_grad.astype(jnp.bfloat16), "seq", scatter_dimension=1, tiled=True
    ).astype(jnp.float32)
    query_back = normalize_back(query_part, query_unit, query_inv)
    key_back = normalize_back(pair_grad[0].reshape(row_count, head_count, HD), key_unit, key_inv)
    qkv_low = jnp.concatenate(
        [
            query_back.reshape(row_count, column_count),
            key_back.reshape(row_count, column_count),
            pair_grad[1],
        ],
        axis=1,
    ).astype(jnp.bfloat16)
    inner_grad = jnp.einsum("rc,dc->rd", qkv_low, full_qkv, preferred_element_type=jnp.float32)
    attended_flat = attended_low.reshape(row_count, column_count)
    share_width = feature_count // lax.axis_size("tensor")
    tensor_count, tensor_at = lax.axis_size("tensor"), lax.axis_index("tensor")

    def share_of(values, owner):
        return lax.dynamic_slice_in_dim(values, owner * share_width, share_width, 1)

    def shifted(values, step):
        pairs = [(place, (place + step) % tensor_count) for place in range(tensor_count)]
        return lax.ppermute(values, "tensor", pairs)

    inner_low = inner_grad.astype(jnp.bfloat16)
    share = share_of(inner_low, tensor_at).astype(jnp.float32)
    for step in range(1, tensor_count):
        sent = share_of(inner_low, (tensor_at + step) % tensor_count)
        share = share + shifted(sent, step).astype(jnp.float32)
    unit_share = share_of(normed, tensor_at)
    own_sums = jnp.stack([jnp.sum(share, axis=-1), jnp.sum(share * unit_share, axis=-1)])
    both_sums = own_sums
    for step in range(1, tensor_count):
        both_sums = both_sums + shifted(own_sums, step)
    means = both_sums[:, :, None] / feature_count
    branch = (share - means[0] - unit_share * means[1]) * inverse
    left_rows = unit_low
    right_rows = grad_rows
    qkv_term = jnp.einsum(
        "rd,rc->dc", left_rows, qkv_low, preferred_element_type=jnp.float32
    ).astype(jnp.bfloat16)
    out_term = jnp.einsum(
        "rd,rc->dc", right_rows, attended_flat, preferred_element_type=jnp.float32
    ).astype(jnp.bfloat16)
    summed = scatter_rows(
        jnp.concatenate([qkv_term, out_term], axis=1).reshape(-1, own_rows, 4 * column_count)
    )
    return (
        summed[:, : 3 * column_count].reshape(own_rows, 3, column_count),
        summed[:, 3 * column_count :],
        branch.astype(jnp.bfloat16)[None],
    )


def solution(mesh):
    return jax.shard_map(
        local,
        mesh=mesh,
        in_specs=(
            P("dp", "seq", None),
            P("dp", "seq", None),
            P(("seq", "dp"), None, "tensor"),
            P(("seq", "dp"), "tensor"),
        ),
        out_specs=(
            P(("seq", "dp"), None, "tensor"),
            P(("seq", "dp"), "tensor"),
            P("dp", "seq", "tensor"),
        ),
        check_vma=False,
    )
```

```python
import functools

import jax
import jax.numpy as jnp
from jax import lax
from jax.experimental import pallas as pl
from jax.experimental.pallas import tpu as pltpu
from jax.sharding import PartitionSpec as P

HD = 128

CORES = 2
CHUNKS = 2
MESH_ID = pl.DeviceIdType.MESH


def greet(seq_count, chip_count, place, chip, core):
    barrier = pltpu.get_barrier_semaphore()

    def signal(device):
        pl.semaphore_signal(barrier, inc=1, device_id=device, device_id_type=MESH_ID)

    @pl.when(place > 0)
    def _():
        signal({"seq": place - 1})

    @pl.when(place < seq_count - 1)
    def _():
        signal({"seq": place + 1})

    for step in range(1, chip_count):
        signal({"dp": (chip + step) % chip_count * CORES + core})
    signal({"dp": chip * CORES + 1 - core})
    ends = jnp.minimum(place, 1) + jnp.minimum(seq_count - 1 - place, 1)
    pl.semaphore_wait(barrier, chip_count + ends)


def gather_kernel(
    seq_count, dp_count, own_ref, out_ref, recv, right_sem, left_sem, chip_sem, core_sem, own_sem
):
    chip_count = dp_count // CORES
    place = lax.axis_index("seq")
    index = lax.axis_index("dp")
    chip, core = index // CORES, index % CORES
    greet(seq_count, chip_count, place, chip, core)
    own_copy = pltpu.make_async_copy(own_ref, out_ref.at[place * dp_count + index], own_sem)
    own_copy.start()

    def copy(source, slot, send_sem, device):
        return pltpu.make_async_remote_copy(
            src_ref=source,
            dst_ref=out_ref.at[slot],
            send_sem=send_sem,
            recv_sem=recv.at[slot],
            device_id=device,
            device_id_type=MESH_ID,
        )

    def right(source, origin):
        return copy(
            source, origin * dp_count + index, right_sem.at[origin], {"seq": place + 1}
        )

    def left(source, origin):
        return copy(source, origin * dp_count + index, left_sem.at[origin], {"seq": place - 1})

    def across(source, origin, step):
        return copy(
            source,
            origin * dp_count + index,
            chip_sem.at[origin * chip_count + step],
            {"dp": (chip + step) % chip_count * CORES + core},
        )

    def beside(source, origin, source_chip):
        return copy(
            source,
            origin * dp_count + source_chip * CORES + core,
            core_sem.at[origin * chip_count + source_chip],
            {"dp": chip * CORES + 1 - core},
        )

    def landed(slot):
        copy(own_ref, slot, core_sem.at[0], {"dp": chip * CORES + 1 - core}).wait_recv()

    def spread(source, origin):
        for step in range(1, chip_count):
            across(source, origin, step).start()
        beside(source, origin, chip).start()

    @pl.when(place < seq_count - 1)
    def _():
        right(own_ref, place).start()

    @pl.when(place > 0)
    def _():
        left(own_ref, place).start()

    spread(own_ref, place)
    for step in range(1, seq_count):
        low, high = place - step, place + step

        @pl.when(low >= 0)
        def _():
            slot = low * dp_count + index
            landed(slot)

            @pl.when(place < seq_count - 1)
            def _():
                right(out_ref.at[slot], low).start()

            spread(out_ref.at[slot], low)

        @pl.when(high < seq_count)
        def _():
            slot = high * dp_count + index
            landed(slot)

            @pl.when(place > 0)
            def _():
                left(out_ref.at[slot], high).start()

            spread(out_ref.at[slot], high)

    for turn in range(seq_count):
        origin = (place + turn) % seq_count
        for step in range(1, chip_count):
            source_chip = (chip + step) % chip_count
            slot = origin * dp_count + source_chip * CORES + core
            landed(slot)
            beside(out_ref.at[slot], origin, source_chip).start()
    for origin in range(seq_count):
        for source_chip in range(chip_count):
            landed(origin * dp_count + source_chip * CORES + 1 - core)
    own_copy.wait()
    for origin in range(seq_count):
        for step in range(1, chip_count):
            across(own_ref, origin, step).wait_send()
        for source_chip in range(chip_count):
            beside(own_ref, origin, source_chip).wait_send()

        @pl.when((origin <= place) & (place < seq_count - 1))
        def _():
            right(own_ref, origin).wait_send()

        @pl.when((origin >= place) & (place > 0))
        def _():
            left(own_ref, origin).wait_send()


def gather_rows(own):
    seq_count, dp_count = lax.axis_size("seq"), lax.axis_size("dp")
    chip_count = dp_count // CORES
    return pl.pallas_call(
        functools.partial(gather_kernel, seq_count, dp_count),
        out_shape=jax.ShapeDtypeStruct((seq_count * dp_count,) + own.shape, own.dtype),
        in_specs=[pl.BlockSpec(memory_space=pltpu.VMEM)],
        out_specs=pl.BlockSpec(memory_space=pl.ANY),
        scratch_shapes=[
            pltpu.SemaphoreType.DMA((seq_count * dp_count,)),
            pltpu.SemaphoreType.DMA((seq_count,)),
            pltpu.SemaphoreType.DMA((seq_count,)),
            pltpu.SemaphoreType.DMA((seq_count * chip_count,)),
            pltpu.SemaphoreType.DMA((seq_count * chip_count,)),
            pltpu.SemaphoreType.DMA,
        ],
        compiler_params=pltpu.CompilerParams(collective_id=0, has_side_effects=True),
        cost_estimate=pl.CostEstimate(flops=0, bytes_accessed=150000000, transcendentals=0),
        name="gather_rows",
    )(own)

def scatter_kernel(
    seq_count,
    dp_count,
    term_ref,
    out_ref,
    held,
    chip_in,
    low_in,
    high_in,
    core_recv,
    core_send,
    chip_recv,
    chip_send,
    low_recv,
    high_recv,
    chain_send,
):
    chip_count = dp_count // CORES
    part_rows = term_ref.shape[1] // CHUNKS
    place = lax.axis_index("seq")
    index = lax.axis_index("dp")
    chip, core = index // CORES, index % CORES
    greet(seq_count, chip_count, place, chip, core)

    def piece(ref, slot, part):
        return ref.at[slot, pl.ds(part * part_rows, part_rows)]

    def copy(source, target_ref, part, slot, send_sem, recv_sem, device):
        return pltpu.make_async_remote_copy(
            src_ref=source,
            dst_ref=piece(target_ref, slot, part),
            send_sem=send_sem.at[slot * CHUNKS + part],
            recv_sem=recv_sem.at[slot * CHUNKS + part],
            device_id=device,
            device_id_type=MESH_ID,
        )

    def beside(part, target, target_chip):
        source = piece(term_ref, target * dp_count + target_chip * CORES + 1 - core, part)
        slot = target * chip_count + target_chip
        device = {"dp": chip * CORES + 1 - core}
        return copy(source, held, part, slot, core_send, core_recv, device)

    def across(part, target, step):
        other = (chip + step) % chip_count
        source = piece(held, target * chip_count + other, part)
        slot = (step - 1) * seq_count + target
        device = {"dp": other * CORES + core}
        return copy(source, chip_in, part, slot, chip_send, chip_recv, device)

    def upward(part, target):
        source = piece(held, target * chip_count + chip, part)
        return copy(source, low_in, part, target, chain_send, low_recv, {"seq": place + 1})

    def downward(part, target):
        source = piece(held, target * chip_count + chip, part)
        return copy(source, high_in, part, target, chain_send, high_recv, {"seq": place - 1})

    def add(slot, part, others):
        @pl.loop(0, part_rows // 16)
        def _(step):
            rows = pl.ds(pl.multiple_of(part * part_rows + step * 16, 16), 16)
            total = held[slot, rows, :].astype(jnp.float32)
            for ref, other in others:
                total = total + ref[other, rows, :].astype(jnp.float32)
            held[slot, rows, :] = total.astype(held.dtype)

    order = []
    for turn in range((seq_count + 1) // 2):
        order.extend(sorted({seq_count - 1 - turn, turn}, reverse=True))
    items = [(part, target) for part in range(CHUNKS) for target in order]
    for part, target in items:
        for step in range(1, chip_count):
            beside(part, target, (chip + step) % chip_count).start()
    for part, target in items:
        beside(part, target, chip).start()
    for part, target in items:
        for step in range(1, chip_count):
            other = (chip + step) % chip_count
            beside(part, target, other).wait_recv()
            own_slot = target * dp_count + other * CORES + core
            add(target * chip_count + other, part, [(term_ref, own_slot)])
            across(part, target, step).start()
    for part, target in items:
        slot = target * chip_count + chip
        others = [(term_ref, target * dp_count + index)]
        beside(part, target, chip).wait_recv()
        for step in range(1, chip_count):
            across(part, target, step).wait_recv()
            others.append((chip_in, (step - 1) * seq_count + target))
        add(slot, part, others)
        if target > 0:

            @pl.when(place < target)
            def _():
                @pl.when(place > 0)
                def _():
                    upward(part, target).wait_recv()
                    add(slot, part, [(low_in, target)])

                upward(part, target).start()

        if target < seq_count - 1:

            @pl.when(place > target)
            def _():
                @pl.when(place < seq_count - 1)
                def _():
                    downward(part, target).wait_recv()
                    add(slot, part, [(high_in, target)])

                downward(part, target).start()

    out_ref[...] = held[place * chip_count + chip].astype(jnp.float32)

    @pl.when(place > 0)
    def _():
        for part in range(CHUNKS):
            upward(part, place).wait_recv()
        out_ref[...] += low_in[place].astype(jnp.float32)

    @pl.when(place < seq_count - 1)
    def _():
        for part in range(CHUNKS):
            downward(part, place).wait_recv()
        out_ref[...] += high_in[place].astype(jnp.float32)

    for part, target in items:
        for step in range(1, chip_count):
            across(part, target, step).wait_send()
        for target_chip in range(chip_count):
            beside(part, target, target_chip).wait_send()

        @pl.when(place != target)
        def _():
            upward(part, target).wait_send()


def scatter_rows(terms):
    seq_count, dp_count = lax.axis_size("seq"), lax.axis_size("dp")
    chip_count = dp_count // CORES
    shape = terms.shape[1:]

    def slots(count):
        return pltpu.VMEM((count,) + shape, terms.dtype)

    def semaphores(count):
        return pltpu.SemaphoreType.DMA((count * CHUNKS,))

    both, peers = seq_count * chip_count, seq_count * (chip_count - 1)
    return pl.pallas_call(
        functools.partial(scatter_kernel, seq_count, dp_count),
        out_shape=jax.ShapeDtypeStruct(shape, jnp.float32),
        in_specs=[pl.BlockSpec(memory_space=pltpu.VMEM)],
        out_specs=pl.BlockSpec(memory_space=pltpu.VMEM),
        scratch_shapes=[
            slots(both),
            slots(peers),
            slots(seq_count),
            slots(seq_count),
            semaphores(both),
            semaphores(both),
            semaphores(peers),
            semaphores(peers),
            semaphores(seq_count),
            semaphores(seq_count),
            semaphores(seq_count),
        ],
        compiler_params=pltpu.CompilerParams(
            collective_id=1, has_side_effects=True, vmem_limit_bytes=40 * 1024 * 1024
        ),
        cost_estimate=pl.CostEstimate(flops=0, bytes_accessed=180000000, transcendentals=0),
        name="scatter_rows",
    )(terms)


epsilon = 1e-06


def normalize(values):
    average = jnp.mean(values, axis=-1, keepdims=True)
    centered = values - average
    inverse = lax.rsqrt(jnp.mean(centered * centered, axis=-1, keepdims=True) + epsilon)
    return (centered * inverse, inverse)


def normalize_back(gradient, normed, inverse):
    mean_grad = jnp.mean(gradient, axis=-1, keepdims=True)
    mean_both = jnp.mean(gradient * normed, axis=-1, keepdims=True)
    return (gradient - mean_grad - normed * mean_both) * inverse


def local(tokens, cotangent, qkv_weight, out_weight):
    row_count = tokens.shape[1]
    feature_count = tokens.shape[2]
    column_count = out_weight.shape[1]
    head_count = column_count // HD
    score_scale = HD ** (-0.5)
    own_rows = qkv_weight.shape[0]
    grad_rows = cotangent[0]
    normed, inverse = normalize(tokens[0].astype(jnp.float32))
    unit_low = normed.astype(jnp.bfloat16)
    flat_weight = qkv_weight.reshape(own_rows, 3 * column_count)
    piece_all = gather_rows(jnp.concatenate([flat_weight, out_weight], axis=1)).reshape(
        feature_count, 4 * column_count
    )
    piece_qkv = piece_all[:, : 3 * column_count]
    piece_out = piece_all[:, 3 * column_count :]
    piece_rows = piece_qkv.shape[0]
    left_rows = unit_low
    right_rows = grad_rows
    projected = jnp.dot(left_rows, piece_qkv, preferred_element_type=jnp.float32)
    attended_grad = jnp.dot(right_rows, piece_out, preferred_element_type=jnp.float32)
    full_qkv = piece_qkv
    projected, attended_grad, full_qkv = (projected, attended_grad, full_qkv)
    query_unit, query_inv = normalize(
        projected[:, :column_count].reshape(row_count, head_count, HD)
    )
    key_unit, key_inv = normalize(
        projected[:, column_count : 2 * column_count].reshape(row_count, head_count, HD)
    )
    query_low = query_unit.astype(jnp.bfloat16)
    key_value = jnp.stack(
        [
            key_unit.astype(jnp.bfloat16).reshape(row_count, column_count),
            projected[:, 2 * column_count :].astype(jnp.bfloat16),
        ]
    )
    grad_low = attended_grad.astype(jnp.bfloat16).reshape(row_count, head_count, HD)

    def scores_of(key_rows):
        piece_rows = key_rows.shape[0]
        return (
            jnp.einsum(
                "qhd,khd->hqk",
                query_low,
                key_rows.reshape(piece_rows, head_count, HD),
                preferred_element_type=jnp.float32,
            )
            * score_scale
        )

    every_pair = lax.all_gather(key_value, "seq", axis=1, tiled=True)
    piece_rows = every_pair.shape[1]
    exponent = jnp.exp(scores_of(every_pair[0]))
    add_exp_total = jnp.sum(exponent, axis=-1)
    weighted = jnp.einsum(
        "hqk,khd->qhd",
        exponent.astype(jnp.bfloat16),
        every_pair[1].reshape(piece_rows, head_count, HD),
        preferred_element_type=jnp.float32,
    )
    exp_total, weighted = (add_exp_total, weighted)
    attended_low = (weighted / exp_total.T[:, :, None]).astype(jnp.bfloat16)
    row_delta = jnp.sum(grad_low.astype(jnp.float32) * attended_low.astype(jnp.float32), axis=-1)
    piece_rows = every_pair.shape[1]
    key_rows = every_pair[0].reshape(piece_rows, head_count, HD)
    value_rows = every_pair[1].reshape(piece_rows, head_count, HD)
    probability = jnp.exp(scores_of(every_pair[0])) / exp_total[:, :, None]
    prob_grad = jnp.einsum("qhd,khd->hqk", grad_low, value_rows, preferred_element_type=jnp.float32)
    grad_score = (probability * (prob_grad - row_delta.T[:, :, None]) * score_scale).astype(
        jnp.bfloat16
    )
    query_part = jnp.einsum(
        "hqk,khd->qhd", grad_score, key_rows, preferred_element_type=jnp.float32
    )
    key_part = jnp.einsum("hqk,qhd->khd", grad_score, query_low, preferred_element_type=jnp.float32)
    value_part = jnp.einsum(
        "hqk,qhd->khd",
        probability.astype(jnp.bfloat16),
        grad_low,
        preferred_element_type=jnp.float32,
    )
    every_grad = jnp.stack(
        [key_part.reshape(piece_rows, column_count), value_part.reshape(piece_rows, column_count)]
    )
    pair_grad = lax.psum_scatter(
        every_grad.astype(jnp.bfloat16), "seq", scatter_dimension=1, tiled=True
    ).astype(jnp.float32)
    query_back = normalize_back(query_part, query_unit, query_inv)
    key_back = normalize_back(pair_grad[0].reshape(row_count, head_count, HD), key_unit, key_inv)
    qkv_low = jnp.concatenate(
        [
            query_back.reshape(row_count, column_count),
            key_back.reshape(row_count, column_count),
            pair_grad[1],
        ],
        axis=1,
    ).astype(jnp.bfloat16)
    inner_grad = jnp.einsum("rc,dc->rd", qkv_low, full_qkv, preferred_element_type=jnp.float32)
    attended_flat = attended_low.reshape(row_count, column_count)
    share_width = feature_count // lax.axis_size("tensor")
    tensor_count, tensor_at = lax.axis_size("tensor"), lax.axis_index("tensor")

    def share_of(values, owner):
        return lax.dynamic_slice_in_dim(values, owner * share_width, share_width, 1)

    def shifted(values, step):
        pairs = [(place, (place + step) % tensor_count) for place in range(tensor_count)]
        return lax.ppermute(values, "tensor", pairs)

    inner_low = inner_grad.astype(jnp.bfloat16)
    arrived = [
        shifted(share_of(inner_low, (tensor_at + step) % tensor_count), step)
        for step in range(1, tensor_count)
    ]
    left_rows = unit_low
    right_rows = grad_rows
    qkv_term = jnp.einsum(
        "rd,rc->dc", left_rows, qkv_low, preferred_element_type=jnp.float32
    ).astype(jnp.bfloat16)
    out_term = jnp.einsum(
        "rd,rc->dc", right_rows, attended_flat, preferred_element_type=jnp.float32
    ).astype(jnp.bfloat16)
    terms = jnp.concatenate([qkv_term, out_term], axis=1)
    terms = terms.reshape(-1, own_rows, 4 * column_count)
    arrived, terms = lax.optimization_barrier((arrived, terms))
    share = share_of(inner_low, tensor_at).astype(jnp.float32)
    for other in arrived:
        share = share + other.astype(jnp.float32)
    unit_share = share_of(normed, tensor_at)
    own_sums = jnp.stack([jnp.sum(share, axis=-1), jnp.sum(share * unit_share, axis=-1)])
    both_sums = own_sums
    for step in range(1, tensor_count):
        both_sums = both_sums + shifted(own_sums, step)
    means = both_sums[:, :, None] / feature_count
    branch = (share - means[0] - unit_share * means[1]) * inverse
    summed = scatter_rows(terms)
    return (
        summed[:, : 3 * column_count].reshape(own_rows, 3, column_count),
        summed[:, 3 * column_count :],
        branch.astype(jnp.bfloat16)[None],
    )


def solution(mesh):
    return jax.shard_map(
        local,
        mesh=mesh,
        in_specs=(
            P("dp", "seq", None),
            P("dp", "seq", None),
            P(("seq", "dp"), None, "tensor"),
            P(("seq", "dp"), "tensor"),
        ),
        out_specs=(
            P(("seq", "dp"), None, "tensor"),
            P(("seq", "dp"), "tensor"),
            P("dp", "seq", "tensor"),
        ),
        check_vma=False,
    )
```
